32 devices in a mesh: seq: 8 (over z, y), head: 4 (over x, core).
Axes of the slice: x: 2, y: 2, z: 4, core: 2. Of those that a mesh axis runs over, the one named last changes fastest.
Arguments:
- cache: bfloat16 [1024, 576], P('seq'), may hold values from -8 to 8
- query_nope: bfloat16 [1024, 4096], P('seq', 'head'), may hold values from -5 to 5
- query_rope: bfloat16 [1024, 2048], P('seq', 'head'), may hold values from -256 to 256
- scale_exp: int32 [1024], P('seq'), may hold values from -1 to 1
- offsets: int32 [16], P('seq'), may hold values from 0 to 960
- up_key: bfloat16 [512, 4096], P(None, 'head'), may hold values from -0.25 to 0.25
- up_value: bfloat16 [512, 4096], P(None, 'head'), may hold values from -0.25 to 0.25
- grad_out: bfloat16 [1024, 4096], P('seq', 'head'), may hold values from -5 to 5
Outputs:
- d_cache: bfloat16 [1024, 576], P('seq')
- d_query_nope: bfloat16 [1024, 4096], P('seq', 'head')
- d_query_rope: bfloat16 [1024, 2048], P('seq', 'head')
The draws below stay inside these ranges and needn't reach their ends.
All inputs are finite; a program needn't handle non-finite values.
Results may differ from the reference program's by a relative error of at most 0.0099.
Values may be sent and summed in bfloat16 or wider, within the bound.
A program may use at most 64 MiB of HBM per device.

```python
import jax
import jax.numpy as jnp
from jax import lax

LATENT = 512
ROPE = 64
NOPE = 128
QBLOCK = 64
HEADS = 32
QUERIES = 1024
KEYS = 1024


def shared_draw(key):
    base = jax.random.fold_in(key, 4049)
    exponents = jax.random.randint(jax.random.fold_in(base, 1), (QUERIES,), -1, 2).astype(jnp.int32)
    return exponents


def draw_scale_exp(key, part):
    exponents = shared_draw(key)
    return exponents


def draw_cache(key, part):
    first = jax.random.fold_in(key, 17)
    latent = jnp.clip(jax.random.normal(jax.random.fold_in(first, 4), (KEYS, LATENT), jnp.float32), -4.0, 4.0)
    rotary = jnp.clip(jax.random.normal(jax.random.fold_in(first, 5), (KEYS, ROPE), jnp.float32), -4.0, 4.0)
    return jnp.concatenate([latent, rotary], axis=1).astype(jnp.bfloat16)


def draw_query_rope(key, part):
    first = jax.random.fold_in(key, 29)
    values = jnp.clip(jax.random.normal(jax.random.fold_in(first, 2), (QUERIES, HEADS * ROPE), jnp.float32), -4.0, 4.0)
    return values.astype(jnp.bfloat16)


def set_ends(array, own_key, least, top_value):
    longest = array.shape.index(max(array.shape))
    spots = []
    for shift in (0, 1):
        where = [jax.random.randint(jax.random.fold_in(own_key, axis), (), 0, length) for axis, length in enumerate(array.shape)]
        where[longest] = (where[longest] + shift) % array.shape[longest]
        spots.append(tuple(where))
    return array.at[spots[0]].set(least).at[spots[1]].set(top_value)


def steps_of(rng, dims, cuts, least, top_value):
    factor_of = 1.0
    for position, blocks in cuts:
        heights = jax.random.uniform(jax.random.fold_in(jax.random.fold_in(rng, 6), position), (blocks,), jnp.float32, least / len(cuts), top_value / len(cuts))
        factor_of = factor_of * jnp.repeat(jnp.exp(heights), dims[position] // blocks).reshape((-1,) + (1,) * (len(dims) - 1 - position))
    return factor_of


def normal_values(key, extent, spread, bound, pieces=(), kind=jnp.bfloat16):
    entries = jax.random.normal(key, extent, jnp.float32) * spread
    if len(pieces) > 0:
        entries = steps_of(key, extent, pieces, -0.22, 0.18) * entries
    return jnp.clip(entries, min=-bound, max=bound).astype(kind)


def setup_inputs(seed: int = 0) -> dict:
    splits = jax.random.split(jax.random.key(seed), 9)
    cache = draw_cache(jax.random.fold_in(splits[8], 71), 0)
    query_nope = normal_values(splits[1], (QUERIES, HEADS * NOPE), 1.0, 5.0, ((0, 8), (1, 4)))
    query_rope = draw_query_rope(jax.random.fold_in(splits[8], 71), 0)
    scale_exp = draw_scale_exp(jax.random.fold_in(splits[8], 71), 0)
    offsets = set_ends(jax.random.randint(splits[4], (QUERIES // QBLOCK,), 0, KEYS - QBLOCK + 1), jax.random.fold_in(splits[4], 1), 0, KEYS - QBLOCK).astype(jnp.int32)
    up_key = normal_values(splits[5], (LATENT, HEADS * NOPE), LATENT ** -0.5, 0.25, ((1, 4),))
    up_value = normal_values(splits[6], (LATENT, HEADS * NOPE), LATENT ** -0.5, 0.25, ((1, 4),))
    grad_out = normal_values(splits[7], (QUERIES, HEADS * NOPE), 1.0, 5.0, ((0, 8), (1, 4)))
    return dict(cache=cache, query_nope=query_nope, query_rope=query_rope, scale_exp=scale_exp, offsets=offsets, up_key=up_key, up_value=up_value, grad_out=grad_out)


def reference(cache, query_nope, query_rope, scale_exp, offsets, up_key, up_value, grad_out):
    scale = (NOPE + ROPE) ** -0.5
    factor = jnp.exp2(scale_exp.astype(jnp.float32))[:, None]
    q_nope = (query_nope.astype(jnp.float32) * factor).astype(jnp.bfloat16).reshape(QUERIES, HEADS, NOPE)
    q_rope = (query_rope.astype(jnp.float32) * factor).astype(jnp.bfloat16).reshape(QUERIES, HEADS, ROPE)
    outgrad = grad_out.reshape(QUERIES, HEADS, NOPE)
    w_key = up_key.reshape(LATENT, HEADS, NOPE)
    w_value = up_value.reshape(LATENT, HEADS, NOPE)
    positions = (offsets[:, None] + jnp.arange(QBLOCK, dtype=jnp.int32)[None, :]).reshape(-1)
    visible = jnp.arange(KEYS, dtype=jnp.int32)[None, :] <= positions[:, None]
    latent = cache[:, :LATENT]

    def one_head(total, items):
        head_nope, head_rope, head_key, head_value, head_grad = items
        absorbed = jnp.dot(head_nope, head_key.T, preferred_element_type=jnp.float32).astype(jnp.bfloat16)
        extended = jnp.concatenate([absorbed, head_rope], axis=1)
        back = jnp.dot(head_grad, head_value.T, preferred_element_type=jnp.float32).astype(jnp.bfloat16)
        raw = jnp.dot(extended, cache.T, preferred_element_type=jnp.float32) * scale
        scores = jnp.where(visible, raw, -jnp.inf)
        top = jnp.max(scores, axis=1, keepdims=True)
        lse = top + jnp.log(jnp.sum(jnp.exp(scores - top), axis=1, keepdims=True))
        probs = jnp.exp(scores - lse)
        probs_b = probs.astype(jnp.bfloat16)
        latent_out = jnp.dot(probs_b, latent, preferred_element_type=jnp.float32)
        delta = jnp.sum(back.astype(jnp.float32) * latent_out, axis=1, keepdims=True)
        dprob = jnp.dot(back, latent.T, preferred_element_type=jnp.float32)
        dscore = (probs * (dprob - delta) * scale).astype(jnp.bfloat16)
        grad_ext = jnp.dot(dscore, cache, preferred_element_type=jnp.float32)
        grad_abs = grad_ext[:, :LATENT].astype(jnp.bfloat16)
        dq_nope = jnp.dot(grad_abs, head_key, preferred_element_type=jnp.float32) * factor
        dq_rope = grad_ext[:, LATENT:] * factor
        term = jnp.dot(dscore.T, extended, preferred_element_type=jnp.float32)
        term_value = jnp.dot(probs_b.T, back, preferred_element_type=jnp.float32)
        total = total + term + jnp.pad(term_value, ((0, 0), (0, ROPE)))
        return total, (dq_nope.astype(jnp.bfloat16), dq_rope.astype(jnp.bfloat16))

    items = (jnp.transpose(q_nope, (1, 0, 2)), jnp.transpose(q_rope, (1, 0, 2)),
             jnp.transpose(w_key, (1, 0, 2)), jnp.transpose(w_value, (1, 0, 2)),
             jnp.transpose(outgrad, (1, 0, 2)))
    start = jnp.zeros((KEYS, LATENT + ROPE), jnp.float32)
    total, (dq_nope, dq_rope) = lax.scan(one_head, start, items)
    d_query_nope = jnp.transpose(dq_nope, (1, 0, 2)).reshape(QUERIES, HEADS * NOPE)
    d_query_rope = jnp.transpose(dq_rope, (1, 0, 2)).reshape(QUERIES, HEADS * ROPE)
    return total.astype(jnp.bfloat16), d_query_nope, d_query_rope
```

```python
import functools
import math

import jax
import jax.numpy as jnp
from jax import lax
from jax.experimental import pallas as pl
from jax.experimental.pallas import tpu as pltpu
from jax.sharding import PartitionSpec as P

LATENT = 512
ROPE = 64
NOPE = 128
QBLOCK = 64
MESH = pl.DeviceIdType.MESH
BF16 = jnp.bfloat16
F32 = jnp.float32
NEG = -1e30


def dot(a, b):
    return jnp.dot(a, b, preferred_element_type=F32)


def dot_nt(a, b):
    return lax.dot_general(a, b, (((1,), (1,)), ((), ())), preferred_element_type=F32)


def flip(v, k):
    bit = 1
    while bit <= k:
        if k & bit:
            v = v + bit - 2 * bit * lax.rem(v // bit, 2)
        bit *= 2
    return v


def kernel(
    nz, nx,
    cache_ref, qn_ref, qr_ref, se_ref, off_ref, uk_ref, uv_ref, go_ref,
    dc_ref, dqn_ref, dqr_ref,
    land, full, cT, extT, ext, backT, back, upkT, S, dP, pT, dsT, mx, D,
    csnd, crcv, psnd, prcv, zsnd, zrcv, wsnd, wrcv, fin,
    g_send, g_recv, c_send, c_recv, p_send, p_recv, z_send, z_recv,
    w_send, w_recv, f_send, f_recv,
):
    width, own = cache_ref.shape
    hwide, qwide = width // 2, width // 4
    half, quarter = own // 2, own // 4
    pair = 2 * own
    queries = qn_ref.shape[0]
    heads = qn_ref.shape[1] // NOPE
    rows = heads * queries
    scale = (NOPE + ROPE) ** (-0.5)
    s_me = lax.axis_index("seq")
    h_me = lax.axis_index("head")
    z, y = s_me // 2, lax.rem(s_me, 2)
    x, core = h_me // 2, lax.rem(h_me, 2)
    xg, xp = x // 2, lax.rem(x, 2)
    oy, oc, oxp = 1 - y, 1 - core, 1 - xp
    ngroups = nx // 2

    def at(zz, yy, xx, cc):
        return (zz * 2 + yy, xx * 2 + cc)

    xo = xg * 2 + oxp
    zs = [flip(z, k) for k in range(nz)]
    z_devs = [at(zz, y, x, core) for zz in zs]
    y_dev = at(z, oy, x, core)
    x_dev = at(z, y, xo, core)
    xy_dev = at(z, oy, xo, core)
    c_dev = at(z, y, x, oc)
    xc_dev = at(z, y, xo, oc)
    xgs = [lax.rem(xg + k, ngroups) for k in range(ngroups)]
    g_devs = [at(z, y, g * 2 + xp, core) for g in xgs]

    barrier = pltpu.get_barrier_semaphore()
    peers = z_devs[1:] + [y_dev, x_dev, xy_dev, c_dev, xc_dev] + g_devs[1:]
    for dev in peers:
        pl.semaphore_signal(barrier, inc=1, device_id=dev, device_id_type=MESH)
    pl.semaphore_wait(barrier, len(peers))

    def remote(src, dst, send, recv, dev):
        return pltpu.make_async_remote_copy(
            src_ref=src, dst_ref=dst, send_sem=send, recv_sem=recv,
            device_id=dev, device_id_type=MESH,
        )

    sends = []

    def go(copy):
        copy.start()
        sends.append(copy)

    counter = [0]

    def part(cc, xx):
        return pl.ds(pl.multiple_of(cc * hwide + xx * qwide, 16), qwide)

    def whole(cc):
        return pl.ds(pl.multiple_of(cc * hwide, 16), hwide)

    def gather(src, blk, rs, slot, dev):
        i = counter[0]
        counter[0] += 1
        go(remote(src, land.at[blk, rs], g_send.at[i], g_recv.at[blk * 4 + slot], dev))

    def arrived(blk, rs, slot):
        remote(
            land.at[blk, rs], land.at[blk, rs], g_send.at[0], g_recv.at[blk * 4 + slot], c_dev
        ).wait_recv()

    mine = part(core, xp)
    for k in range(1, nz):
        gather(cache_ref.at[mine], s_me, mine, 0, z_devs[k])
    gather(cache_ref.at[whole(core)], s_me, whole(core), 0, y_dev)

    land[s_me] = cache_ref[...]

    def block(k, yy):
        return zs[k] * 2 + yy

    def e_own():
        blk = block(0, oy)
        arrived(blk, whole(core), 0)
        gather(land.at[blk, whole(core)], blk, whole(core), 2, c_dev)

    def e_z(k):
        blk = block(k, y)
        arrived(blk, mine, 0)
        gather(land.at[blk, mine], blk, mine, 0, y_dev)
        gather(land.at[blk, mine], blk, mine, 1, x_dev)

    def e_y(k):
        blk = block(k, oy)
        arrived(blk, mine, 0)
        gather(land.at[blk, mine], blk, mine, 1, x_dev)

    def e_x(k, yy):
        blk = block(k, yy)
        arrived(blk, part(core, oxp), 1)
        gather(land.at[blk, whole(core)], blk, whole(core), 2, c_dev)

    def e_c(k):
        if k:
            arrived(block(k, y), whole(oc), 2)
        arrived(block(k, oy), whole(oc), 2)

    factor = jnp.exp2(se_ref[...].astype(F32))
    lane = lax.broadcasted_iota(jnp.int32, (1, queries), 1)
    pos = jnp.zeros((1, queries), jnp.int32)
    for b in range(queries // QBLOCK):
        inside = (lane >= b * QBLOCK) & (lane < (b + 1) * QBLOCK)
        pos = jnp.where(inside, off_ref[b] + lane - b * QBLOCK, pos)

    for h in range(heads):
        cols = slice(h * NOPE, (h + 1) * NOPE)
        qs = slice(h * queries, (h + 1) * queries)
        w = uk_ref[:, cols]
        a = (dot_nt(w, qn_ref[:, cols]) * factor).astype(BF16)
        extT[0:LATENT, qs] = a
        ext[qs, 0:LATENT] = a.T
        upkT[cols, :] = w.T
        g = dot_nt(uv_ref[:, cols], go_ref[:, cols]).astype(BF16)
        backT[:, qs] = g
        back[qs, :] = g.T
    for h in range(0, heads, 2):
        r = (qr_ref[:, h * ROPE : (h + 2) * ROPE].astype(F32).T * factor).astype(BF16)
        for i in range(2):
            p = r[i * ROPE : (i + 1) * ROPE, :]
            qs = slice((h + i) * queries, (h + i + 1) * queries)
            extT[LATENT:width, qs] = p
            ext[qs, LATENT:width] = p.astype(F32).T.astype(BF16)
    mx[...] = jnp.full(mx.shape, NEG, F32)

    tile = 2 * queries
    pos2 = jnp.concatenate([pos, pos], axis=1)
    tiles = rows // tile

    def base_of(k):
        return pl.multiple_of(zs[k] * pair, pair)

    def turn(k):
        for yy in range(2):
            at_col = pl.ds(pl.multiple_of((zs[k] * 2 + yy) * own, own), own)
            b = land[zs[k] * 2 + yy]
            cT[:, at_col] = b
            full[at_col, :] = b.T

    def scores(k, t):
        base = base_of(k)
        c = full[pl.ds(base, pair), :]
        key = base + lax.broadcasted_iota(jnp.int32, (pair, tile), 0)
        seen = key <= pos2
        ls = slice(t * tile, (t + 1) * tile)
        s = dot(c, extT[:, ls]) * (scale * math.log2(math.e))
        s = jnp.where(seen, s, NEG)
        S[pl.ds(base, pair), ls] = s
        mx[:, ls] = jnp.maximum(mx[:, ls], jnp.max(s.reshape(pair // 8, 8, tile), axis=0))
        dP[pl.ds(base, pair), ls] = dot(c[:, :LATENT], backT[:, ls])

    events = [functools.partial(e_z, 1), e_own]
    events += [functools.partial(e_z, k) for k in range(2, nz)]
    work = []
    for k in range(1, nz):
        events += [functools.partial(e_y, k), functools.partial(e_x, k, y)]
    late = [functools.partial(e_x, k, oy) for k in range(1, nz)]

    def pieces(k):
        def first():
            e_c(k)
            turn(k)
            scores(k, 0)

        return [first] + [functools.partial(scores, k, t) for t in range(1, tiles)]

    for e in events[:nz]:
        e()
    work = pieces(0)
    rest = events[nz:]
    while rest:
        rest.pop(0)()
        if work:
            work.pop(0)()
    for w_ in work:
        w_()
    for k in range(1, nz):
        late.pop(0)()
        if k > 1:
            for p in pieces(k - 1):
                p()
    for p in pieces(nz - 1):
        p()

    keys = full.shape[0]
    chunk = own

    def soften(h, carry):
        ls = pl.ds(pl.multiple_of(h * queries, queries), queries)
        top = jnp.max(mx[:, ls], axis=0, keepdims=True)
        tot = jnp.zeros((8, queries), F32)
        dl = jnp.zeros((8, queries), F32)
        for i in range(keys // chunk):
            rs = slice(i * chunk, (i + 1) * chunk)
            p = jnp.exp2(S[rs, ls] - top)
            S[rs, ls] = p
            tot = tot + jnp.sum(p.reshape(chunk // 8, 8, queries), axis=0)
            dl = dl + jnp.sum((p * dP[rs, ls]).reshape(chunk // 8, 8, queries), axis=0)
        inv = 1.0 / jnp.sum(tot, axis=0, keepdims=True)
        delta = jnp.sum(dl, axis=0, keepdims=True) * inv
        for i in range(keys // chunk):
            rs = slice(i * chunk, (i + 1) * chunk)
            pr = S[rs, ls] * inv
            pT[rs, ls] = pr.astype(BF16)
            dsT[rs, ls] = (pr * (dP[rs, ls] - delta) * scale).astype(BF16)
        return carry

    lax.fori_loop(0, heads, soften, 0)

    def span(zz, yy, cc, xx=None):
        start = (zz * 2 + yy) * own + cc * half
        if xx is None:
            return pl.ds(pl.multiple_of(start, half), half)
        return pl.ds(pl.multiple_of(start + xx * quarter, quarter), quarter)

    def core_copy(k):
        return remote(csnd.at[k], crcv.at[k], c_send.at[k], c_recv.at[k], c_dev)

    plane = [(oy, xp, y_dev), (y, oxp, x_dev), (oy, oxp, xy_dev)]

    def plane_copy(k, i):
        return remote(
            psnd.at[k, i], prcv.at[k, i], p_send.at[k * 3 + i], p_recv.at[k * 3 + i], plane[i][2]
        )

    def z_copy(k):
        return remote(zsnd.at[k], zrcv.at[k], z_send.at[k], z_recv.at[k], z_devs[k])

    def step_d(k):
        rs = pl.ds(base_of(k), pair)
        ds, pb = dsT[rs, :], pT[rs, :]
        D[rs, 0:LATENT] = dot(ds, ext[:, 0:LATENT]) + dot(pb, back[...])
        D[rs, LATENT:width] = dot(ds, ext[:, LATENT:width])
        for yy in range(2):
            csnd[k, yy] = D[span(zs[k], yy, oc), :].astype(BF16)
        go(core_copy(k))

    def quarter_of(k, yy, xx):
        rs = pl.ds(pl.multiple_of(xx * quarter, quarter), quarter)
        return D[span(zs[k], yy, core, xx), :] + crcv[k, yy, rs, :].astype(F32)

    def step_e(k):
        core_copy(k).wait_recv()
        for i in (2, 0, 1):
            yy, xx, _ = plane[i]
            psnd[k, i] = quarter_of(k, yy, xx).astype(BF16)
            go(plane_copy(k, i))

    def step_f(k):
        u = quarter_of(k, y, xp)
        for i in range(3):
            plane_copy(k, i).wait_recv()
            u = u + prcv[k, i].astype(F32)
        if k:
            zsnd[k] = u.astype(BF16)
            go(z_copy(k))
        return u

    def grads(h):
        g = dot(cT[...], dsT[:, h * queries : (h + 2) * queries])
        lo = g[0:LATENT].astype(BF16)
        hi = g[LATENT:width]
        ropes = []
        for i in range(2):
            qs = slice(i * queries, (i + 1) * queries)
            cols = slice((h + i) * NOPE, (h + i + 1) * NOPE)
            d = dot(upkT[cols, :], lo[:, qs]) * factor
            dqn_ref[:, cols] = d.T.astype(BF16)
            ropes.append(hi[:, qs] * factor)
        dqr_ref[:, h * ROPE : (h + 2) * ROPE] = jnp.concatenate(ropes, axis=0).T.astype(BF16)

    order = list(range(nz - 1, -1, -1))
    todo = list(range(0, heads, 2))
    ready_e, ready_f = [], []
    for i, k in enumerate(order):
        step_d(k)
        if i > 0:
            step_e(order[i - 1])
        if i > 2:
            step_f(order[i - 3])
    grads(todo.pop(0))
    step_e(order[-1])
    for k in order[max(0, nz - 3) : -1]:
        step_f(k)
        if todo:
            grads(todo.pop(0))
    while todo:
        grads(todo.pop(0))
    v = step_f(0)
    for k in range(1, nz):
        z_copy(k).wait_recv()
        v = v + zrcv[k].astype(F32)
    if ngroups > 1:
        wsnd[...] = v.astype(BF16)
        for k in range(1, ngroups):
            go(remote(wsnd, wrcv.at[xg], w_send.at[k], w_recv.at[xg], g_devs[k]))
        wrcv[xg] = v.astype(BF16)
        for k in range(1, ngroups):
            remote(wsnd, wrcv.at[xgs[k]], w_send.at[k], w_recv.at[xgs[k]], g_devs[k]).wait_recv()
        v = wrcv[0].astype(F32)
        for i in range(1, ngroups):
            v = v + wrcv[i].astype(F32)
    here = pl.ds(pl.multiple_of(core * half + xp * quarter, quarter), quarter)
    fin[here, :] = v.astype(BF16)
    last = [(core, oxp, x_dev), (oc, oxp, xc_dev), (oc, xp, c_dev)]
    for i, (_, _, dev) in enumerate(last):
        go(remote(fin.at[here], fin.at[here], f_send.at[i], f_recv.at[i], dev))
    for i, (cc, xx, dev) in enumerate(last):
        there = pl.ds(pl.multiple_of(cc * half + xx * quarter, quarter), quarter)
        remote(fin.at[there], fin.at[there], f_send.at[i], f_recv.at[i], dev).wait_recv()
    dc_ref[...] = fin[...].T
    for copy in sends:
        copy.wait_send()


def finish(a, b, c, oa, ob, oc, sem):
    copies = [
        pltpu.make_async_copy(src, dst, sem.at[i])
        for i, (src, dst) in enumerate(((b, ob), (a, oa), (c, oc)))
    ]
    for copy in copies:
        copy.start()
    for copy in copies:
        copy.wait()


def solution(mesh):
    seq, head = mesh.shape["seq"], mesh.shape["head"]
    nz, nx = seq // 2, head // 2

    def per_device(cache, qn, qr, se, off, uk, uv, go):
        own, width = cache.shape
        half, quarter = own // 2, own // 4
        keys = own * seq
        queries = qn.shape[0]
        heads = qn.shape[1] // NOPE
        rows = heads * queries
        vm = pltpu.VMEM
        dma = pltpu.SemaphoreType.DMA
        vspec = pl.BlockSpec(memory_space=pltpu.VMEM)
        sspec = pl.BlockSpec(memory_space=pltpu.SMEM)
        hspec = pl.BlockSpec(memory_space=pl.ANY)
        shapes = ((width, own), qn.shape, qr.shape)
        out = pl.pallas_call(
            functools.partial(kernel, nz, nx),
            out_shape=tuple(vm(s, BF16) for s in shapes),
            in_specs=[vspec, vspec, vspec, vspec, sspec, vspec, vspec, vspec],
            out_specs=(vspec, vspec, vspec),
            scratch_shapes=[
                vm((seq, width, own), BF16), vm((keys, width), BF16), vm((width, keys), BF16),
                vm((width, rows), BF16), vm((rows, width), BF16),
                vm((LATENT, rows), BF16), vm((rows, LATENT), BF16),
                vm((heads * NOPE, LATENT), BF16),
                vm((keys, rows), F32), vm((keys, rows), F32),
                vm((keys, rows), BF16), vm((keys, rows), BF16),
                vm((8, rows), F32), vm((keys, width), F32),
                vm((nz, 2, half, width), BF16), vm((nz, 2, half, width), BF16),
                vm((nz, 3, quarter, width), BF16), vm((nz, 3, quarter, width), BF16),
                vm((nz, quarter, width), BF16), vm((nz, quarter, width), BF16),
                vm((quarter, width), BF16), vm((nx // 2, quarter, width), BF16),
                vm((own, width), BF16),
                dma((8 * nz,)), dma((4 * seq,)), dma((nz,)), dma((nz,)),
                dma((3 * nz,)), dma((3 * nz,)), dma((nz,)), dma((nz,)),
                dma((nx // 2,)), dma((nx // 2,)), dma((3,)), dma((3,)),
            ],
            compiler_params=pltpu.CompilerParams(
                collective_id=0, has_side_effects=True, vmem_limit_bytes=58 * 1024 * 1024
            ),
        )(cache.T, qn, qr, se.reshape(1, -1), off, uk, uv, go)
        dc, dqn, dqr = pl.pallas_call(
            finish,
            out_shape=tuple(jax.ShapeDtypeStruct(s, BF16) for s in shapes),
            in_specs=[vspec] * 3,
            out_specs=(hspec,) * 3,
            scratch_shapes=[dma((3,))],
            compiler_params=pltpu.CompilerParams(vmem_limit_bytes=1024 * 1024),
        )(*out)
        return dc.T, dqn, dqr

    in_specs = (
        P("seq", None), P("seq", "head"), P("seq", "head"), P("seq"), P("seq"),
        P(None, "head"), P(None, "head"), P("seq", "head"),
    )
    out_specs = (P("seq", None), P("seq", "head"), P("seq", "head"))
    return jax.shard_map(
        per_device, mesh=mesh, in_specs=in_specs, out_specs=out_specs, check_vma=False
    )
```

```python
import functools
import math

import jax
import jax.numpy as jnp
from jax import lax
from jax.experimental import pallas as pl
from jax.experimental.pallas import tpu as pltpu
from jax.sharding import PartitionSpec as P

LATENT = 512
ROPE = 64
NOPE = 128
QBLOCK = 64
MESH = pl.DeviceIdType.MESH
BF16 = jnp.bfloat16
F32 = jnp.float32
NEG = -1e30


def dot(a, b):
    return jnp.dot(a, b, preferred_element_type=F32)


def dot_nt(a, b):
    return lax.dot_general(a, b, (((1,), (1,)), ((), ())), preferred_element_type=F32)


def flip(v, k):
    bit = 1
    while bit <= k:
        if k & bit:
            v = v + bit - 2 * bit * lax.rem(v // bit, 2)
        bit *= 2
    return v


def kernel(
    nz, nx,
    cache_hbm, qn_hbm, qr_hbm, se_hbm, off_hbm, uk_hbm, uv_hbm, go_hbm,
    dc_ref, dqn_ref, dqr_ref,
    cache_ref, qn_ref, qr_ref, se_ref, off_ref, uk_ref, uv_ref, go_ref,
    land, full, cT, extT, ext, backT, back, upkT, S, dP, pT, dsT, mx, tot, dl, D,
    csnd, crcv, psnd, prcv, zsnd, zrcv, wsnd, wrcv, fin,
    in_sem, g_send, g_recv, c_send, c_recv, p_send, p_recv, z_send, z_recv,
    w_send, w_recv, f_send, f_recv,
):
    width, own = cache_ref.shape
    hwide, qwide = width // 2, width // 4
    half, quarter = own // 2, own // 4
    pair = 2 * own
    queries = qn_ref.shape[0]
    heads = qn_ref.shape[1] // NOPE
    rows = heads * queries
    scale = (NOPE + ROPE) ** (-0.5)
    s_me = lax.axis_index("seq")
    h_me = lax.axis_index("head")
    z, y = s_me // 2, lax.rem(s_me, 2)
    x, core = h_me // 2, lax.rem(h_me, 2)
    xg, xp = x // 2, lax.rem(x, 2)
    oy, oc, oxp = 1 - y, 1 - core, 1 - xp
    ngroups = nx // 2

    loads = [
        pltpu.make_async_copy(src, dst, in_sem.at[i])
        for i, (src, dst) in enumerate((
            (cache_hbm, cache_ref), (se_hbm, se_ref), (off_hbm, off_ref), (qn_hbm, qn_ref),
            (uk_hbm, uk_ref), (go_hbm, go_ref), (uv_hbm, uv_ref), (qr_hbm, qr_ref),
        ))
    ]
    loads[0].start()

    def at(zz, yy, xx, cc):
        return (zz * 2 + yy, xx * 2 + cc)

    xo = xg * 2 + oxp
    zs = [flip(z, k) for k in range(nz)]
    z_devs = [at(zz, y, x, core) for zz in zs]
    y_dev = at(z, oy, x, core)
    x_dev = at(z, y, xo, core)
    xy_dev = at(z, oy, xo, core)
    c_dev = at(z, y, x, oc)
    xc_dev = at(z, y, xo, oc)
    xgs = [lax.rem(xg + k, ngroups) for k in range(ngroups)]
    g_devs = [at(z, y, g * 2 + xp, core) for g in xgs]

    barrier = pltpu.get_barrier_semaphore()
    peers = z_devs[1:] + [y_dev, x_dev, xy_dev, c_dev, xc_dev] + g_devs[1:]
    for dev in peers:
        pl.semaphore_signal(barrier, inc=1, device_id=dev, device_id_type=MESH)
    for load in loads[1:]:
        load.start()
    loads[0].wait()
    pl.semaphore_wait(barrier, len(peers))

    def remote(src, dst, send, recv, dev):
        return pltpu.make_async_remote_copy(
            src_ref=src, dst_ref=dst, send_sem=send, recv_sem=recv,
            device_id=dev, device_id_type=MESH,
        )

    sends = []

    def go(copy):
        copy.start()
        sends.append(copy)

    counter = [0]

    def part(cc, xx):
        return pl.ds(pl.multiple_of(cc * hwide + xx * qwide, 16), qwide)

    def whole(cc):
        return pl.ds(pl.multiple_of(cc * hwide, 16), hwide)

    mine, theirs = part(core, xp), part(core, oxp)

    def gather(src, k, yy, rs, slot, dev):
        i = counter[0]
        counter[0] += 1
        blk = k * 2 + yy
        go(remote(src, land.at[blk, rs], g_send.at[i], g_recv.at[blk * 4 + slot], dev))

    def pass_on(k, yy, rs, slot, dev):
        gather(land.at[k * 2 + yy, rs], k, yy, rs, slot, dev)

    def arrived(k, yy, rs, slot):
        blk = k * 2 + yy
        remote(
            land.at[blk, rs], land.at[blk, rs], g_send.at[0], g_recv.at[blk * 4 + slot], c_dev
        ).wait_recv()

    for k in list(range(1, nz)):
        gather(cache_ref.at[mine], k, y, mine, 0, z_devs[k])
    gather(cache_ref.at[whole(core)], 0, y, whole(core), 0, y_dev)
    land[y] = cache_ref[...]

    def e_own():
        arrived(0, oy, whole(core), 0)
        pass_on(0, oy, whole(core), 2, c_dev)

    def e_z(k):
        arrived(k, y, mine, 0)
        pass_on(k, y, mine, 1, x_dev)
        pass_on(k, y, mine, 0, y_dev)
        pass_on(k, y, mine, 1, xy_dev)

    def e_h(k):
        arrived(k, y, theirs, 1)
        pass_on(k, y, whole(core), 2, c_dev)
        arrived(k, oy, mine, 0)
        arrived(k, oy, theirs, 1)
        pass_on(k, oy, whole(core), 2, c_dev)

    def e_c(k):
        if k:
            arrived(k, y, whole(oc), 2)
        arrived(k, oy, whole(oc), 2)

    loads[1].wait()
    loads[2].wait()
    factor = jnp.exp2(se_ref[...].astype(F32))
    lane = lax.broadcasted_iota(jnp.int32, (1, queries), 1)
    pos = jnp.zeros((1, queries), jnp.int32)
    for b in range(queries // QBLOCK):
        inside = (lane >= b * QBLOCK) & (lane < (b + 1) * QBLOCK)
        pos = jnp.where(inside, off_ref[b] + lane - b * QBLOCK, pos)
    for load in loads[3:]:
        load.wait()

    for h in range(heads):
        cols = slice(h * NOPE, (h + 1) * NOPE)
        qs = slice(h * queries, (h + 1) * queries)
        w = uk_ref[:, cols]
        a = (dot_nt(w, qn_ref[:, cols]) * factor).astype(BF16)
        extT[0:LATENT, qs] = a
        ext[qs, 0:LATENT] = a.T
        upkT[cols, :] = w.T
        g = dot_nt(uv_ref[:, cols], go_ref[:, cols]).astype(BF16)
        backT[:, qs] = g
        back[qs, :] = g.T
    for h in range(0, heads, 2):
        r = (qr_ref[:, h * ROPE : (h + 2) * ROPE].astype(F32).T * factor).astype(BF16)
        for i in range(2):
            p = r[i * ROPE : (i + 1) * ROPE, :]
            qs = slice((h + i) * queries, (h + i + 1) * queries)
            extT[LATENT:width, qs] = p
            ext[qs, LATENT:width] = p.astype(F32).T.astype(BF16)

    tile = 2 * queries
    pos2 = jnp.concatenate([pos, pos], axis=1)
    tiles = rows // tile

    def turn(k):
        for yy in range(2):
            cols = slice(k * pair + yy * own, k * pair + (yy + 1) * own)
            b = land[k * 2 + yy]
            cT[:, cols] = b
            full[cols, :] = b.T

    def scores(k, first, last):
        rs = slice(k * pair, (k + 1) * pair)
        c = full[rs, :]
        key = zs[k] * pair + lax.broadcasted_iota(jnp.int32, (pair, tile), 0)
        seen = key <= pos2
        for t in range(first, last):
            ls = slice(t * tile, (t + 1) * tile)
            s = dot(c, extT[:, ls]) * (scale * math.log2(math.e))
            s = jnp.where(seen, s, NEG)
            S[rs, ls] = s
            mx[k, :, ls] = jnp.max(s.reshape(pair // 8, 8, tile), axis=0)
            dP[rs, ls] = dot(c[:, :LATENT], backT[:, ls])

    def soft(k, t):
        ls = slice(t * tile, (t + 1) * tile)
        top = jnp.max(mx[k, :, ls], axis=0, keepdims=True)
        t8 = jnp.zeros((8, tile), F32)
        d8 = jnp.zeros((8, tile), F32)
        for i in range(2):
            n = pair // 2
            rs = slice(k * pair + i * n, k * pair + (i + 1) * n)
            p = jnp.exp2(S[rs, ls] - top)
            S[rs, ls] = p
            t8 = t8 + jnp.sum(p.reshape(n // 8, 8, tile), axis=0)
            d8 = d8 + jnp.sum((p * dP[rs, ls]).reshape(n // 8, 8, tile), axis=0)
        tot[k, :, ls] = t8
        dl[k, :, ls] = d8

    def both(k, first, last):
        for t in range(first, last):
            scores(k, t, t + 1)
            if t > first:
                soft(k, t - 1)
        soft(k, last - 1)

    ks = list(range(1, nz))
    e_z(ks[0])
    e_own()
    for k in ks[1:]:
        e_z(k)
    e_c(0)
    turn(0)
    both(0, 0, tiles)
    e_h(ks[0])
    for i, k in enumerate(ks):
        for kk in ks[i + 1 : i + 2]:
            e_h(kk)
        e_c(k)
        turn(k)
        both(k, 0, tiles)
    tops = [jnp.max(mx[k], axis=0, keepdims=True) for k in range(nz)]
    top = functools.reduce(jnp.maximum, tops)
    parts = [jnp.exp2(t - top) for t in tops]
    total = sum(p * jnp.sum(tot[k], axis=0, keepdims=True) for k, p in enumerate(parts))
    delta = sum(p * jnp.sum(dl[k], axis=0, keepdims=True) for k, p in enumerate(parts))
    inv = 1.0 / total
    delta = delta * inv

    def settle(k, i):
        f = parts[k] * inv
        for h in range(heads):
            ls = slice(h * queries, (h + 1) * queries)
            rs = slice(k * pair + i * own, k * pair + (i + 1) * own)
            pr = S[rs, ls] * f[:, ls]
            pT[rs, ls] = pr.astype(BF16)
            dsT[rs, ls] = (pr * (dP[rs, ls] - delta[:, ls]) * scale).astype(BF16)

    def step_piece(k, yy):
        rs = slice(k * pair + yy * own, k * pair + (yy + 1) * own)
        ds, pb = dsT[rs, :], pT[rs, :]
        v = dot(ds, ext[:, 0:LATENT]) + dot(pb, back[...])
        t = dot(ds, ext[:, LATENT:width])
        n = quarter // 2
        for c in range(2):
            for xx in range(2):
                r = c * half + xx * quarter
                for j in range(LATENT // 128):
                    cols = slice(j * 128, (j + 1) * 128)
                    D[k, yy, c, xx, j * quarter : (j + 1) * quarter, :] = v[r : r + quarter, cols]
                tail = jnp.concatenate([t[r : r + n], t[r + n : r + quarter]], axis=1)
                D[k, yy, c, xx, LATENT // 128 * quarter :, :] = tail

    def core_copy(k):
        return remote(csnd.at[k], crcv.at[k], c_send.at[k], c_recv.at[k], c_dev)

    plane = [(oy, xp, y_dev), (y, oxp, x_dev), (oy, oxp, xy_dev)]

    def plane_copy(k, i):
        return remote(
            psnd.at[k, i], prcv.at[k, i], p_send.at[k * 3 + i], p_recv.at[k * 3 + i], plane[i][2]
        )

    def z_copy(k):
        return remote(zsnd.at[k], zrcv.at[k], z_send.at[k], z_recv.at[k], z_devs[k])

    def step_d(k, then):
        for yy in range(2):
            step_piece(k, yy)
            if then is not None:
                settle(then, yy)
        for yy in range(2):
            csnd[k, yy] = D[k, yy, oc].astype(BF16)
        go(core_copy(k))

    def chip_sum(k, yy, xx):
        return D[k, yy, core, xx] + crcv[k, yy, xx].astype(F32)

    def step_e(k):
        core_copy(k).wait_recv()
        for i in (2, 0, 1):
            yy, xx, _ = plane[i]
            psnd[k, i] = chip_sum(k, yy, xx).astype(BF16)
            go(plane_copy(k, i))

    def step_f(k):
        u = chip_sum(k, y, xp)
        for i in range(3):
            plane_copy(k, i).wait_recv()
            u = u + prcv[k, i].astype(F32)
        if k:
            zsnd[k] = u.astype(BF16)
            go(z_copy(k))
        return u

    def grad_ext(h):
        cols = slice(h * queries, (h + 2) * queries)
        g = dot(cT[...], dsT[:, cols])
        extT[0:LATENT, cols] = g[0:LATENT].astype(BF16)
        hi = g[LATENT:width]
        ropes = [hi[:, i * queries : (i + 1) * queries] * factor for i in range(2)]
        dqr_ref[:, h * ROPE : (h + 2) * ROPE] = jnp.concatenate(ropes, axis=0).T.astype(BF16)

    def grad_nope(h):
        for i in range(h, h + 2):
            cols = slice(i * NOPE, (i + 1) * NOPE)
            d = dot(upkT[cols, :], extT[0:LATENT, i * queries : (i + 1) * queries]) * factor
            dqn_ref[:, cols] = d.T.astype(BF16)

    todo = [functools.partial(grad_ext, 0)]
    for h in range(2, heads, 2):
        todo += [functools.partial(grad_ext, h), functools.partial(grad_nope, h - 2)]
    todo += [functools.partial(grad_nope, heads - 2)]

    def some(n):
        for _ in range(n):
            if todo:
                todo.pop(0)()

    order = list(range(nz - 1, -1, -1))
    settle(order[0], 0)
    settle(order[0], 1)
    waiting = list(order[:-1])
    for i, k in enumerate(order):
        step_d(k, order[i + 1] if i + 1 < nz else None)
        if i > 0:
            step_e(order[i - 1])
        if i > 3:
            step_f(waiting.pop(0))
    some(1)
    step_e(0)
    for i, k in enumerate(waiting):
        some((1, 1, 1)[i] if i < len((1, 1, 1)) else 0)
        step_f(k)
    some(1)
    v = step_f(0)
    for k in range(nz - 1, 0, -1):
        z_copy(k).wait_recv()
        v = v + zrcv[k].astype(F32)
    if ngroups > 1:
        wsnd[...] = v.astype(BF16)
        for k in range(1, ngroups):
            go(remote(wsnd, wrcv.at[xg], w_send.at[k], w_recv.at[xg], g_devs[k]))
        wrcv[xg] = v.astype(BF16)
        for k in range(1, ngroups):
            remote(wsnd, wrcv.at[xgs[k]], w_send.at[k], w_recv.at[xgs[k]], g_devs[k]).wait_recv()
        v = wrcv[0].astype(F32)
        for i in range(1, ngroups):
            v = v + wrcv[i].astype(F32)
    fin[core * 2 + xp] = v.astype(BF16)
    here = fin.at[core * 2 + xp]
    last = [(core, oxp, x_dev), (oc, oxp, xc_dev), (oc, xp, c_dev)]
    for i, (_, _, dev) in enumerate(last):
        go(remote(here, here, f_send.at[i], f_recv.at[i], dev))
    some(len(todo))
    for copy in sends[: -len(last)]:
        copy.wait_send()
    for i, (cc, xx, dev) in enumerate(last):
        there = fin.at[cc * 2 + xx]
        remote(there, there, f_send.at[i], f_recv.at[i], dev).wait_recv()
    quarters = [fin[i].astype(F32) for i in range(4)]
    for j in range(LATENT // 128):
        rs = slice(j * quarter, (j + 1) * quarter)
        tall = jnp.concatenate([q[rs] for q in quarters], axis=0)
        dc_ref[j * 128 : (j + 1) * 128, :] = tall.T.astype(BF16)
    rs = slice(LATENT // 128 * quarter, quarter * width // 128)
    tails = [q[rs, i * ROPE : (i + 1) * ROPE] for q in quarters for i in range(2)]
    dc_ref[LATENT:width, :] = jnp.concatenate(tails, axis=0).T.astype(BF16)
    for copy in sends[-len(last) :]:
        copy.wait_send()


def finish(a, b, c, oa, ob, oc, sem):
    copies = [
        pltpu.make_async_copy(src, dst, sem.at[i])
        for i, (src, dst) in enumerate(((b, ob), (a, oa), (c, oc)))
    ]
    for copy in copies:
        copy.start()
    for copy in copies:
        copy.wait()


def solution(mesh):
    seq, head = mesh.shape["seq"], mesh.shape["head"]
    nz, nx = seq // 2, head // 2

    def per_device(cache, qn, qr, se, off, uk, uv, go):
        own, width = cache.shape
        keys = own * seq
        prow = own // 4 * width // 128
        queries = qn.shape[0]
        heads = qn.shape[1] // NOPE
        rows = heads * queries
        vm = pltpu.VMEM
        dma = pltpu.SemaphoreType.DMA
        vspec = pl.BlockSpec(memory_space=pltpu.VMEM)
        hspec = pl.BlockSpec(memory_space=pl.ANY)
        shapes = ((width, own), qn.shape, qr.shape)
        out = pl.pallas_call(
            functools.partial(kernel, nz, nx),
            out_shape=tuple(vm(s, BF16) for s in shapes),
            in_specs=[hspec] * 8,
            out_specs=(vspec, vspec, vspec),
            scratch_shapes=[
                vm((width, own), BF16), vm(qn.shape, BF16), vm(qr.shape, BF16),
                vm((1, queries), jnp.int32), pltpu.SMEM(off.shape, jnp.int32),
                vm(uk.shape, BF16), vm(uv.shape, BF16), vm(go.shape, BF16),
                vm((seq, width, own), BF16), vm((keys, width), BF16), vm((width, keys), BF16),
                vm((width, rows), BF16), vm((rows, width), BF16),
                vm((LATENT, rows), BF16), vm((rows, LATENT), BF16),
                vm((heads * NOPE, LATENT), BF16),
                vm((keys, rows), F32), vm((keys, rows), F32),
                vm((keys, rows), BF16), vm((keys, rows), BF16),
                vm((nz, 8, rows), F32), vm((nz, 8, rows), F32), vm((nz, 8, rows), F32),
                vm((nz, 2, 2, 2, prow, 128), F32),
                vm((nz, 2, 2, prow, 128), BF16), vm((nz, 2, 2, prow, 128), BF16),
                vm((nz, 3, prow, 128), BF16), vm((nz, 3, prow, 128), BF16),
                vm((nz, prow, 128), BF16), vm((nz, prow, 128), BF16),
                vm((prow, 128), BF16), vm((nx // 2, prow, 128), BF16),
                vm((4, prow, 128), BF16),
                dma((8,)), dma((6 * nz + 4,)), dma((4 * seq,)), dma((nz,)), dma((nz,)),
                dma((3 * nz,)), dma((3 * nz,)), dma((nz,)), dma((nz,)),
                dma((nx // 2,)), dma((nx // 2,)), dma((3,)), dma((3,)),
            ],
            compiler_params=pltpu.CompilerParams(
                collective_id=0, has_side_effects=True, vmem_limit_bytes=58 * 1024 * 1024
            ),
        )(cache.T, qn, qr, se.reshape(1, -1), off, uk, uv, go)
        dc, dqn, dqr = pl.pallas_call(
            finish,
            out_shape=tuple(jax.ShapeDtypeStruct(s, BF16) for s in shapes),
            in_specs=[vspec] * 3,
            out_specs=(hspec,) * 3,
            scratch_shapes=[dma((3,))],
            compiler_params=pltpu.CompilerParams(vmem_limit_bytes=1024 * 1024),
        )(*out)
        return dc.T, dqn, dqr

    in_specs = (
        P("seq", None), P("seq", "head"), P("seq", "head"), P("seq"), P("seq"),
        P(None, "head"), P(None, "head"), P("seq", "head"),
    )
    out_specs = (P("seq", None), P("seq", "head"), P("seq", "head"))
    return jax.shard_map(
        per_device, mesh=mesh, in_specs=in_specs, out_specs=out_specs, check_vma=False
    )
```

```python
import functools
import math

import jax
import jax.numpy as jnp
from jax import lax
from jax.experimental import pallas as pl
from jax.experimental.pallas import tpu as pltpu
from jax.sharding import PartitionSpec as P

LATENT = 512
ROPE = 64
NOPE = 128
QBLOCK = 64
MESH = pl.DeviceIdType.MESH
BF16 = jnp.bfloat16
F32 = jnp.float32
NEG = -1e30


def dot(a, b):
    return jnp.dot(a, b, preferred_element_type=F32)


def dot_nt(a, b):
    return lax.dot_general(a, b, (((1,), (1,)), ((), ())), preferred_element_type=F32)


def flip(v, k):
    bit = 1
    while bit <= k:
        if k & bit:
            v = v + bit - 2 * bit * lax.rem(v // bit, 2)
        bit *= 2
    return v


def kernel(
    nz, nx,
    cache_hbm, qn_hbm, qr_hbm, se_hbm, off_hbm, uk_hbm, uv_hbm, go_hbm,
    dc_ref, dqn_ref, dqr_ref,
    cache_ref, qr_ref, se_ref, off_ref, wide,
    land, full, cT, extT, ext, backT, back, upkT, S, dP, pT, dsT, mx, tot, dl, D,
    csnd, crcv, psnd, prcv, zsnd, zrcv, wsnd, wrcv, fin,
    in_sem, g_send, g_recv, c_send, c_recv, p_send, p_recv, z_send, z_recv,
    w_send, w_recv, f_send, f_recv,
):
    width, own = cache_ref.shape
    hwide, qwide = width // 2, width // 4
    half, quarter = own // 2, own // 4
    pair = 2 * own
    queries = qn_hbm.shape[0]
    heads = qn_hbm.shape[1] // NOPE
    qn_ref, go_ref = wide.at[0:queries], wide.at[queries : 2 * queries]
    uk_ref = wide.at[2 * queries : 2 * queries + LATENT]
    uv_ref = wide.at[2 * queries + LATENT :]
    rows = heads * queries
    scale = (NOPE + ROPE) ** (-0.5)
    s_me = lax.axis_index("seq")
    h_me = lax.axis_index("head")
    z, y = s_me // 2, lax.rem(s_me, 2)
    x, core = h_me // 2, lax.rem(h_me, 2)
    xg, xp = x // 2, lax.rem(x, 2)
    oy, oc, oxp = 1 - y, 1 - core, 1 - xp
    ngroups = nx // 2

    places = (
        (cache_hbm, cache_ref, 0), (se_hbm, se_ref, 1), (off_hbm, off_ref, 2), (qr_hbm, qr_ref, 3),
        (qn_hbm, qn_ref, 4), (uk_hbm, uk_ref, 4), (go_hbm, go_ref, 4), (uv_hbm, uv_ref, 4),
    )
    loads = [pltpu.make_async_copy(src, dst, in_sem.at[i]) for src, dst, i in places]
    loads[0].start()

    def at(zz, yy, xx, cc):
        return (zz * 2 + yy, xx * 2 + cc)

    xo = xg * 2 + oxp
    zs = [flip(z, k) for k in range(nz)]
    z_devs = [at(zz, y, x, core) for zz in zs]
    y_dev = at(z, oy, x, core)
    x_dev = at(z, y, xo, core)
    xy_dev = at(z, oy, xo, core)
    c_dev = at(z, y, x, oc)
    xc_dev = at(z, y, xo, oc)
    xgs = [lax.rem(xg + k, ngroups) for k in range(ngroups)]
    g_devs = [at(z, y, g * 2 + xp, core) for g in xgs]

    barrier = pltpu.get_barrier_semaphore()
    peers = z_devs[1:] + [y_dev, x_dev, xy_dev, c_dev, xc_dev] + g_devs[1:]
    for dev in peers:
        pl.semaphore_signal(barrier, inc=1, device_id=dev, device_id_type=MESH)
    for load in loads[1:]:
        load.start()
    loads[0].wait()
    pl.semaphore_wait(barrier, len(peers))

    def remote(src, dst, send, recv, dev):
        return pltpu.make_async_remote_copy(
            src_ref=src, dst_ref=dst, send_sem=send, recv_sem=recv,
            device_id=dev, device_id_type=MESH,
        )

    def go(copy):
        copy.start()

    def sent(ref, sem):
        remote(ref, ref, sem, sem, c_dev).wait_send()

    def part(cc, xx):
        return pl.ds(pl.multiple_of(cc * hwide + xx * qwide, 16), qwide)

    def whole(cc):
        return pl.ds(pl.multiple_of(cc * hwide, 16), hwide)

    mine, theirs = part(core, xp), part(core, oxp)

    def gather(src, k, r, rs, sem, dev):
        go(remote(src, land.at[k * 2 + r, rs], g_send.at[0], g_recv.at[sem], dev))

    def pass_on(k, r, rs, sem, dev, to=None):
        gather(land.at[k * 2 + r, rs], k, r if to is None else to, rs, sem, dev)

    def arrived(k, r, rs, sem):
        piece = land.at[k * 2 + r, rs]
        remote(piece, piece, g_send.at[0], g_recv.at[sem], c_dev).wait_recv()

    arrivals = [(0, 0), (0, 1)] + [(k, r) for r in range(2) for k in range(1, nz)]
    groups = [arrivals[i : i + 2] for i in range(0, len(arrivals), 2)]
    group_of = {b: g for g, blocks in enumerate(groups) for b in blocks}

    def from_plane(k, r):
        return nz + k * 2 + r

    def from_core(k, r):
        return 3 * nz + group_of[k, r]

    for k in range(1, nz):
        gather(cache_ref.at[mine], k, 0, mine, k, z_devs[k])
    gather(cache_ref.at[whole(core)], 0, 1, whole(core), 0, y_dev)
    land[0] = cache_ref[...]

    def e_own():
        arrived(0, 1, whole(core), 0)
        pass_on(0, 1, whole(core), from_core(0, 1), c_dev)

    def e_z(k):
        arrived(k, 0, mine, k)
        pass_on(k, 0, mine, from_plane(k, 0), x_dev)
        pass_on(k, 0, mine, from_plane(k, 1), y_dev, 1)
        if k in range(1, nz):
            pass_on(k, 0, mine, from_plane(k, 1), xy_dev, 1)

    def e_h(k, r):
        arrived(k, r, whole(core) if r else theirs, from_plane(k, r))
        if r == 0 and k not in range(1, nz):
            pass_on(k, 0, theirs, from_plane(k, 1), y_dev, 1)
        pass_on(k, r, whole(core), from_core(k, r), c_dev)

    loads[1].wait()
    loads[2].wait()
    factor = jnp.exp2(se_ref[...].astype(F32))
    lane = lax.broadcasted_iota(jnp.int32, (1, queries), 1)
    pos = jnp.zeros((1, queries), jnp.int32)
    for b in range(queries // QBLOCK):
        inside = (lane >= b * QBLOCK) & (lane < (b + 1) * QBLOCK)
        pos = jnp.where(inside, off_ref[b] + lane - b * QBLOCK, pos)
    loads[3].wait()
    pltpu.make_async_copy(wide, wide, in_sem.at[4]).wait()

    for h in range(heads):
        cols = slice(h * NOPE, (h + 1) * NOPE)
        qs = slice(h * queries, (h + 1) * queries)
        w = uk_ref[:, cols]
        a = (dot_nt(w, qn_ref[:, cols]) * factor).astype(BF16)
        extT[0:LATENT, qs] = a
        ext[qs, 0:LATENT] = a.T
        upkT[cols, :] = w.T
        g = dot_nt(uv_ref[:, cols], go_ref[:, cols]).astype(BF16)
        backT[:, qs] = g
        back[qs, :] = g.T
    for h in range(0, heads, 2):
        r = (qr_ref[:, h * ROPE : (h + 2) * ROPE].astype(F32).T * factor).astype(BF16)
        for i in range(2):
            p = r[i * ROPE : (i + 1) * ROPE, :]
            qs = slice((h + i) * queries, (h + i + 1) * queries)
            extT[LATENT:width, qs] = p
            ext[qs, LATENT:width] = p.astype(F32).T.astype(BF16)

    tile = 2 * queries
    pos2 = jnp.concatenate([pos, pos], axis=1)
    tiles = rows // tile

    def rows_of(k, r):
        return slice((k * 2 + r) * own, (k * 2 + r + 1) * own)

    def turn(k, r):
        b = land[k * 2 + r]
        cT[:, rows_of(k, r)] = b
        full[rows_of(k, r), :] = b.T

    def scores(g, t):
        c = jnp.concatenate([full[rows_of(*b), :] for b in groups[g]], axis=0)
        ls = slice(t * tile, (t + 1) * tile)
        s = dot(c, extT[:, ls]) * (scale * math.log2(math.e))
        dp = dot(c[:, :LATENT], backT[:, ls])
        m = jnp.full((8, tile), NEG, F32)
        for i, (k, r) in enumerate(groups[g]):
            base = (zs[k] * 2 + (oy if r else y)) * own
            key = base + lax.broadcasted_iota(jnp.int32, (own, tile), 0)
            si = jnp.where(key <= pos2, s[i * own : (i + 1) * own], NEG)
            S[rows_of(k, r), ls] = si
            m = jnp.maximum(m, jnp.max(si.reshape(own // 8, 8, tile), axis=0))
            dP[rows_of(k, r), ls] = dp[i * own : (i + 1) * own]
        mx[g, :, ls] = m

    def soft(g, t):
        ls = slice(t * tile, (t + 1) * tile)
        top = jnp.max(mx[g, :, ls], axis=0, keepdims=True)
        t8 = jnp.zeros((8, tile), F32)
        d8 = jnp.zeros((8, tile), F32)
        for b in groups[g]:
            rs = rows_of(*b)
            p = jnp.exp2(S[rs, ls] - top)
            S[rs, ls] = p
            t8 = t8 + jnp.sum(p.reshape(own // 8, 8, tile), axis=0)
            d8 = d8 + jnp.sum((p * dP[rs, ls]).reshape(own // 8, 8, tile), axis=0)
        tot[g, :, ls] = t8
        dl[g, :, ls] = d8

    def both(g, first, last):
        for t in range(first, last):
            scores(g, t)
            if t > first:
                soft(g, t - 1)
        soft(g, last - 1)

    def ready(g):
        first = groups[g][0]
        if g == 0:
            arrived(0, 1, whole(oc), from_core(0, 1))
        else:
            two = land.at[0:2, whole(oc)]
            remote(two, two, g_send.at[0], g_recv.at[from_core(*first)], c_dev).wait_recv()
        for b in groups[g]:
            turn(*b)

    e_z(1)
    e_own()
    for k in range(2, nz):
        e_z(k)
    pending = arrivals[2:]

    def forward(g):
        while pending and group_of[pending[0]] <= g:
            e_h(*pending.pop(0))

    ready(0)
    both(0, 0, tiles)
    forward(1)
    for g in range(1, len(groups)):
        forward(g + 1)
        ready(g)
        both(g, 0, tiles)

    tops = [jnp.max(mx[k], axis=0, keepdims=True) for k in range(nz)]
    top = functools.reduce(jnp.maximum, tops)
    parts = [jnp.exp2(t - top) for t in tops]
    total = sum(p * jnp.sum(tot[k], axis=0, keepdims=True) for k, p in enumerate(parts))
    delta = sum(p * jnp.sum(dl[k], axis=0, keepdims=True) for k, p in enumerate(parts))
    inv = 1.0 / total
    delta = delta * inv

    def settle(k, r):
        f = parts[group_of[k, r]] * inv
        rs = rows_of(k, r)
        for h in range(heads):
            ls = slice(h * queries, (h + 1) * queries)
            pr = S[rs, ls] * f[:, ls]
            pT[rs, ls] = pr.astype(BF16)
            dsT[rs, ls] = (pr * (dP[rs, ls] - delta[:, ls]) * scale).astype(BF16)

    def step_piece(k, r):
        rs = rows_of(k, r)
        ds, pb = dsT[rs, :], pT[rs, :]
        v = dot(ds, ext[:, 0:LATENT]) + dot(pb, back[...])
        t = dot(ds, ext[:, LATENT:width])
        n = quarter // 2
        for c in range(2):
            for xx in range(2):
                i = c * half + xx * quarter
                for j in range(LATENT // 128):
                    cols = slice(j * 128, (j + 1) * 128)
                    D[k, r, c, xx, j * quarter : (j + 1) * quarter, :] = v[i : i + quarter, cols]
                tail = jnp.concatenate([t[i : i + n], t[i + n : i + quarter]], axis=1)
                D[k, r, c, xx, LATENT // 128 * quarter :, :] = tail

    parts_of = [((k, r),) for k in range(nz - 1, nz - 1, -1) for r in (1, 0)]
    parts_of += [((k, 1), (k, 0)) for k in range(nz - 1, -1, -1)]

    def core_copy(i):
        k, r = parts_of[i][0]
        at_ = (k,) if len(parts_of[i]) > 1 else (k, r)
        return remote(csnd.at[at_], crcv.at[at_], c_send.at[0], c_recv.at[i], c_dev)

    plane = [(1, xp, y_dev), (0, oxp, x_dev), (1, oxp, xy_dev)]

    def plane_copy(k, i):
        return remote(
            psnd.at[k, i], prcv.at[k, i], p_send.at[0], p_recv.at[k], plane[i][2]
        )

    def z_copy(k):
        return remote(zsnd.at[k], zrcv.at[k], z_send.at[0], z_recv.at[0], z_devs[k])

    def chip_sum(k, r, xx):
        return D[k, r, core, xx] + crcv[k, r, xx].astype(F32)

    def step_d(i):
        then = list(parts_of[i + 1]) if i + 1 < len(parts_of) else []
        for b in parts_of[i]:
            step_piece(*b)
            if then:
                settle(*then.pop(0))
        for b in then:
            settle(*b)
        for k, r in parts_of[i]:
            csnd[k, r] = D[k, r, oc].astype(BF16)
        go(core_copy(i))

    def step_e(i):
        core_copy(i).wait_recv()
        for j in (2, 0, 1):
            for k, r in parts_of[i]:
                if plane[j][0] == r:
                    psnd[k, j] = chip_sum(k, r, plane[j][1]).astype(BF16)
                    go(plane_copy(k, j))

    def step_f(k):
        remote(prcv.at[k], prcv.at[k], p_send.at[0], p_recv.at[k], c_dev).wait_recv()
        u = chip_sum(k, 0, xp)
        for i in range(3):
            u = u + prcv[k, i].astype(F32)
        if k:
            zsnd[k] = u.astype(BF16)
            go(z_copy(k))
        return u

    def grad_ext(h):
        cols = slice(h * queries, (h + 2) * queries)
        g = dot(cT[...], dsT[:, cols])
        extT[0:LATENT, cols] = g[0:LATENT].astype(BF16)
        hi = g[LATENT:width]
        ropes = [hi[:, i * queries : (i + 1) * queries] * factor for i in range(2)]
        dqr_ref[:, h * ROPE : (h + 2) * ROPE] = jnp.concatenate(ropes, axis=0).T.astype(BF16)

    def grad_nope(h):
        for i in range(h, h + 2):
            cols = slice(i * NOPE, (i + 1) * NOPE)
            d = dot(upkT[cols, :], extT[0:LATENT, i * queries : (i + 1) * queries]) * factor
            dqn_ref[:, cols] = d.T.astype(BF16)

    todo = [functools.partial(grad_ext, 0)]
    for h in range(2, heads, 2):
        todo += [functools.partial(grad_ext, h), functools.partial(grad_nope, h - 2)]
    todo += [functools.partial(grad_nope, heads - 2)]

    def some(n):
        for _ in range(n):
            if todo:
                todo.pop(0)()

    for b in parts_of[0]:
        settle(*b)
    waiting = list(range(nz - 1, 0, -1))
    done = 0
    for i in range(len(parts_of)):
        step_d(i)
        while done < i and (len(parts_of[done + 1]) > 1 or done + 1 < i):
            step_e(done)
            done += 1
        if nz > 4 and i > nz:
            step_f(waiting.pop(0))
    some(1)
    for i in range(done, len(parts_of) - 1):
        step_e(i)
    for i, k in enumerate(waiting):
        if 1 and i == 2:
            step_e(len(parts_of) - 1)
        some((1, 1, 1)[i] if i < len((1, 1, 1)) else 0)
        step_f(k)
    some(2)
    v = step_f(0)
    if nz > 1:
        others = zrcv.at[1:nz]
        remote(others, others, z_send.at[0], z_recv.at[0], c_dev).wait_recv()
    for k in range(nz - 1, 0, -1):
        v = v + zrcv[k].astype(F32)
    if ngroups > 1:
        wsnd[...] = v.astype(BF16)
        for k in range(1, ngroups):
            go(remote(wsnd, wrcv.at[xg], w_send.at[k], w_recv.at[xg], g_devs[k]))
        wrcv[xg] = v.astype(BF16)
        for k in range(1, ngroups):
            remote(wsnd, wrcv.at[xgs[k]], w_send.at[k], w_recv.at[xgs[k]], g_devs[k]).wait_recv()
        v = wrcv[0].astype(F32)
        for i in range(1, ngroups):
            v = v + wrcv[i].astype(F32)
    fin[core * 2 + xp] = v.astype(BF16)
    here = fin.at[core * 2 + xp]
    last = [x_dev, xc_dev, c_dev]
    for dev in last:
        go(remote(here, here, f_send.at[0], f_recv.at[0], dev))
    some(len(todo))
    sent(land.at[0 : 2 * nz - 1], g_send.at[0])
    sent(csnd, c_send.at[0])
    sent(psnd, p_send.at[0])
    if nz > 1:
        sent(zsnd.at[1:nz], z_send.at[0])
    for k in range(1, ngroups):
        sent(wsnd, w_send.at[k])
    remote(fin.at[0:3], fin.at[0:3], f_send.at[0], f_recv.at[0], c_dev).wait_recv()
    quarters = [fin[i].astype(F32) for i in range(4)]
    for j in range(LATENT // 128):
        rs = slice(j * quarter, (j + 1) * quarter)
        tall = jnp.concatenate([q[rs] for q in quarters], axis=0)
        dc_ref[j * 128 : (j + 1) * 128, :] = tall.T.astype(BF16)
    rs = slice(LATENT // 128 * quarter, quarter * width // 128)
    tails = [q[rs, i * ROPE : (i + 1) * ROPE] for q in quarters for i in range(2)]
    dc_ref[LATENT:width, :] = jnp.concatenate(tails, axis=0).T.astype(BF16)
    sent(fin.at[0:3], f_send.at[0])


def finish(a, b, c, oa, ob, oc, sem):
    copies = [
        pltpu.make_async_copy(src, dst, sem.at[i])
        for i, (src, dst) in enumerate(((b, ob), (a, oa), (c, oc)))
    ]
    for copy in copies:
        copy.start()
    for copy in copies:
        copy.wait()


def solution(mesh):
    seq, head = mesh.shape["seq"], mesh.shape["head"]
    nz, nx = seq // 2, head // 2

    def per_device(cache, qn, qr, se, off, uk, uv, go):
        own, width = cache.shape
        keys = own * seq
        prow = own // 4 * width // 128
        queries = qn.shape[0]
        heads = qn.shape[1] // NOPE
        rows = heads * queries
        vm = pltpu.VMEM
        dma = pltpu.SemaphoreType.DMA
        vspec = pl.BlockSpec(memory_space=pltpu.VMEM)
        hspec = pl.BlockSpec(memory_space=pl.ANY)
        shapes = ((width, own), qn.shape, qr.shape)
        out = pl.pallas_call(
            functools.partial(kernel, nz, nx),
            out_shape=tuple(vm(s, BF16) for s in shapes),
            in_specs=[hspec] * 8,
            out_specs=(vspec, vspec, vspec),
            scratch_shapes=[
                vm((width, own), BF16), vm(qr.shape, BF16),
                vm((1, queries), jnp.int32), pltpu.SMEM(off.shape, jnp.int32),
                vm((2 * (queries + LATENT), qn.shape[1]), BF16),
                vm((seq, width, own), BF16), vm((keys, width), BF16), vm((width, keys), BF16),
                vm((width, rows), BF16), vm((rows, width), BF16),
                vm((LATENT, rows), BF16), vm((rows, LATENT), BF16),
                vm((heads * NOPE, LATENT), BF16),
                vm((keys, rows), F32), vm((keys, rows), F32),
                vm((keys, rows), BF16), vm((keys, rows), BF16),
                vm((nz, 8, rows), F32), vm((nz, 8, rows), F32), vm((nz, 8, rows), F32),
                vm((nz, 2, 2, 2, prow, 128), F32),
                vm((nz, 2, 2, prow, 128), BF16), vm((nz, 2, 2, prow, 128), BF16),
                vm((nz, 3, prow, 128), BF16), vm((nz, 3, prow, 128), BF16),
                vm((nz, prow, 128), BF16), vm((nz, prow, 128), BF16),
                vm((prow, 128), BF16), vm((nx // 2, prow, 128), BF16),
                vm((4, prow, 128), BF16),
                dma((5,)), dma((1,)), dma((4 * nz,)), dma((1,)), dma((2 * nz,)),
                dma((1,)), dma((nz,)), dma((1,)), dma((1,)),
                dma((nx // 2,)), dma((nx // 2,)), dma((1,)), dma((1,)),
            ],
            compiler_params=pltpu.CompilerParams(
                collective_id=0, has_side_effects=True, vmem_limit_bytes=58 * 1024 * 1024
            ),
        )(cache.T, qn, qr, se.reshape(1, -1), off, uk, uv, go)
        dc, dqn, dqr = pl.pallas_call(
            finish,
            out_shape=tuple(jax.ShapeDtypeStruct(s, BF16) for s in shapes),
            in_specs=[vspec] * 3,
            out_specs=(hspec,) * 3,
            scratch_shapes=[dma((3,))],
            compiler_params=pltpu.CompilerParams(vmem_limit_bytes=1024 * 1024),
        )(*out)
        return dc.T, dqn, dqr

    in_specs = (
        P("seq", None), P("seq", "head"), P("seq", "head"), P("seq"), P("seq"),
        P(None, "head"), P(None, "head"), P("seq", "head"),
    )
    out_specs = (P("seq", None), P("seq", "head"), P("seq", "head"))
    return jax.shard_map(
        per_device, mesh=mesh, in_specs=in_specs, out_specs=out_specs, check_vma=False
    )
```

```python
import functools
import math

import jax
import jax.numpy as jnp
from jax import lax
from jax.experimental import pallas as pl
from jax.experimental.pallas import tpu as pltpu
from jax.sharding import PartitionSpec as P

LATENT = 512
ROPE = 64
NOPE = 128
QBLOCK = 64
MESH = pl.DeviceIdType.MESH
BF16 = jnp.bfloat16
F32 = jnp.float32
NEG = -1e30


def dot(a, b):
    return jnp.dot(a, b, preferred_element_type=F32)


def dot_nt(a, b):
    return lax.dot_general(a, b, (((1,), (1,)), ((), ())), preferred_element_type=F32)


def flip(v, k):
    bit = 1
    while bit <= k:
        if k & bit:
            v = v + bit - 2 * bit * lax.rem(v // bit, 2)
        bit *= 2
    return v


def kernel(
    nz, nx,
    cache_hbm, qn_hbm, qr_hbm, se_hbm, off_hbm, uk_hbm, uv_hbm, go_hbm,
    dc_ref, dqn_ref, dqr_ref,
    cache_ref, qr_ref, se_ref, off_ref, wide,
    land, full, cT, extT, ext, backT, back, upkT, S, dP, pT, dsT, mx, tot, dl, D,
    csnd, crcv, psnd, prcv, zsnd, zrcv, wsnd, wrcv, fin,
    in_sem, g_send, g_recv, c_send, c_recv, p_send, p_recv, z_send, z_recv,
    w_send, w_recv, f_send, f_recv,
):
    width, own = cache_ref.shape
    hwide, qwide = width // 2, width // 4
    half, quarter = own // 2, own // 4
    pair = 2 * own
    queries = qn_hbm.shape[0]
    heads = qn_hbm.shape[1] // NOPE
    qn_ref, go_ref = wide.at[0:queries], wide.at[queries : 2 * queries]
    uk_ref = wide.at[2 * queries : 2 * queries + LATENT]
    uv_ref = wide.at[2 * queries + LATENT :]
    rows = heads * queries
    scale = (NOPE + ROPE) ** (-0.5)
    s_me = lax.axis_index("seq")
    h_me = lax.axis_index("head")
    z, y = s_me // 2, lax.rem(s_me, 2)
    x, core = h_me // 2, lax.rem(h_me, 2)
    xg, xp = x // 2, lax.rem(x, 2)
    oy, oc, oxp = 1 - y, 1 - core, 1 - xp
    ngroups = nx // 2

    places = (
        (cache_hbm, cache_ref, 0), (se_hbm, se_ref, 1), (off_hbm, off_ref, 2), (qr_hbm, qr_ref, 3),
        (qn_hbm, qn_ref, 4), (uk_hbm, uk_ref, 4), (go_hbm, go_ref, 4), (uv_hbm, uv_ref, 4),
    )
    loads = [pltpu.make_async_copy(src, dst, in_sem.at[i]) for src, dst, i in places]
    loads[0].start()

    def at(zz, yy, xx, cc):
        return (zz * 2 + yy, xx * 2 + cc)

    xo = xg * 2 + oxp
    zs = [flip(z, k) for k in range(nz)]
    z_devs = [at(zz, y, x, core) for zz in zs]
    y_dev = at(z, oy, x, core)
    x_dev = at(z, y, xo, core)
    xy_dev = at(z, oy, xo, core)
    c_dev = at(z, y, x, oc)
    xc_dev = at(z, y, xo, oc)
    xgs = [lax.rem(xg + k, ngroups) for k in range(ngroups)]
    g_devs = [at(z, y, g * 2 + xp, core) for g in xgs]

    barrier = pltpu.get_barrier_semaphore()
    peers = z_devs[1:] + [y_dev, x_dev, xy_dev, c_dev, xc_dev] + g_devs[1:]
    for dev in peers:
        pl.semaphore_signal(barrier, inc=1, device_id=dev, device_id_type=MESH)
    for load in loads[1:]:
        load.start()
    loads[0].wait()
    pl.semaphore_wait(barrier, len(peers))

    def remote(src, dst, send, recv, dev):
        return pltpu.make_async_remote_copy(
            src_ref=src, dst_ref=dst, send_sem=send, recv_sem=recv,
            device_id=dev, device_id_type=MESH,
        )

    def go(copy):
        copy.start()

    def sent(ref, sem):
        remote(ref, ref, sem, sem, c_dev).wait_send()

    def part(cc, xx):
        return pl.ds(pl.multiple_of(cc * hwide + xx * qwide, 16), qwide)

    def whole(cc):
        return pl.ds(pl.multiple_of(cc * hwide, 16), hwide)

    mine, theirs = part(core, xp), part(core, oxp)

    def gather(src, k, r, rs, sem, dev):
        go(remote(src, land.at[k * 2 + r, rs], g_send.at[0], g_recv.at[sem], dev))

    def pass_on(k, r, rs, sem, dev, to=None):
        gather(land.at[k * 2 + r, rs], k, r if to is None else to, rs, sem, dev)

    def arrived(k, r, rs, sem):
        piece = land.at[k * 2 + r, rs]
        remote(piece, piece, g_send.at[0], g_recv.at[sem], c_dev).wait_recv()

    arrivals = [(0, 0), (0, 1)] + [(k, r) for r in range(2) for k in range(1, nz)]
    groups = [arrivals[i : i + 2] for i in range(0, len(arrivals), 2)]
    group_of = {b: g for g, blocks in enumerate(groups) for b in blocks}

    def from_plane(k, r):
        return nz + (k - 1) * 2 + r

    def from_core(k, r):
        return 3 * nz - 2 + group_of[k, r]

    gather(cache_ref.at[mine], 1, 0, mine, 1, z_devs[1])
    gather(cache_ref.at[whole(core)], 0, 1, whole(core), 0, y_dev)
    for k in range(2, nz):
        gather(cache_ref.at[mine], k, 0, mine, k, z_devs[k])
    land[0] = cache_ref[...]

    def e_own():
        arrived(0, 1, whole(core), 0)
        pass_on(0, 1, whole(core), from_core(0, 1), c_dev)

    def e_z(k):
        arrived(k, 0, mine, k)
        pass_on(k, 0, mine, from_plane(k, 0), x_dev)
        pass_on(k, 0, mine, from_plane(k, 1), y_dev, 1)
        if k in range(1, nz):
            pass_on(k, 0, mine, from_plane(k, 1), xy_dev, 1)

    def e_h(k, r):
        arrived(k, r, whole(core) if r else theirs, from_plane(k, r))
        if r == 0 and k not in range(1, nz):
            pass_on(k, 0, theirs, from_plane(k, 1), y_dev, 1)
        pass_on(k, r, whole(core), from_core(k, r), c_dev)

    loads[1].wait()
    loads[2].wait()
    factor = jnp.exp2(se_ref[...].astype(F32))
    lane = lax.broadcasted_iota(jnp.int32, (1, queries), 1)
    pos = jnp.zeros((1, queries), jnp.int32)
    for b in range(queries // QBLOCK):
        inside = (lane >= b * QBLOCK) & (lane < (b + 1) * QBLOCK)
        pos = jnp.where(inside, off_ref[b] + lane - b * QBLOCK, pos)
    loads[3].wait()
    pltpu.make_async_copy(wide, wide, in_sem.at[4]).wait()

    for h in range(heads):
        cols = slice(h * NOPE, (h + 1) * NOPE)
        qs = slice(h * queries, (h + 1) * queries)
        w = uk_ref[:, cols]
        a = (dot_nt(w, qn_ref[:, cols]) * factor).astype(BF16)
        extT[0:LATENT, qs] = a
        ext[qs, 0:LATENT] = a.T
        upkT[cols, :] = w.T
        g = dot_nt(uv_ref[:, cols], go_ref[:, cols]).astype(BF16)
        backT[:, qs] = g
        back[qs, :] = g.T
    for h in range(0, heads, 2):
        r = (qr_ref[:, h * ROPE : (h + 2) * ROPE].astype(F32).T * factor).astype(BF16)
        for i in range(2):
            p = r[i * ROPE : (i + 1) * ROPE, :]
            qs = slice((h + i) * queries, (h + i + 1) * queries)
            extT[LATENT:width, qs] = p
            ext[qs, LATENT:width] = p.astype(F32).T.astype(BF16)

    tile = 2 * queries
    pos2 = jnp.concatenate([pos, pos], axis=1)
    tiles = rows // tile

    def rows_of(k, r):
        return slice((k * 2 + r) * own, (k * 2 + r + 1) * own)

    def turn(k, r):
        b = land[k * 2 + r]
        cT[:, rows_of(k, r)] = b
        full[rows_of(k, r), :] = b.T

    def scores(g, t):
        c = jnp.concatenate([full[rows_of(*b), :] for b in groups[g]], axis=0)
        ls = slice(t * tile, (t + 1) * tile)
        s = dot(c, extT[:, ls]) * (scale * math.log2(math.e))
        dp = dot(c[:, :LATENT], backT[:, ls])
        m = jnp.full((8, tile), NEG, F32)
        for i, (k, r) in enumerate(groups[g]):
            base = (zs[k] * 2 + (oy if r else y)) * own
            key = base + lax.broadcasted_iota(jnp.int32, (own, tile), 0)
            si = jnp.where(key <= pos2, s[i * own : (i + 1) * own], NEG)
            S[rows_of(k, r), ls] = si
            m = jnp.maximum(m, jnp.max(si.reshape(own // 8, 8, tile), axis=0))
            dP[rows_of(k, r), ls] = dp[i * own : (i + 1) * own]
        mx[g, :, ls] = m

    def soft(g, t):
        ls = slice(t * tile, (t + 1) * tile)
        top = jnp.max(mx[g, :, ls], axis=0, keepdims=True)
        t8 = jnp.zeros((8, tile), F32)
        d8 = jnp.zeros((8, tile), F32)
        for b in groups[g]:
            rs = rows_of(*b)
            p = jnp.exp2(S[rs, ls] - top)
            S[rs, ls] = p
            t8 = t8 + jnp.sum(p.reshape(own // 8, 8, tile), axis=0)
            d8 = d8 + jnp.sum((p * dP[rs, ls]).reshape(own // 8, 8, tile), axis=0)
        tot[g, :, ls] = t8
        dl[g, :, ls] = d8

    def both(g, first, last):
        for t in range(first, last):
            scores(g, t)
            if t > first:
                soft(g, t - 1)
        soft(g, last - 1)

    def ready(g):
        first = groups[g][0]
        if g == 0:
            arrived(0, 1, whole(oc), from_core(0, 1))
        else:
            two = land.at[0:2, whole(oc)]
            remote(two, two, g_send.at[0], g_recv.at[from_core(*first)], c_dev).wait_recv()
        for b in groups[g]:
            turn(*b)

    e_z(1)
    e_own()
    for k in range(2, nz):
        e_z(k)
    pending = arrivals[2:]

    def forward(g):
        while pending and group_of[pending[0]] <= g:
            e_h(*pending.pop(0))

    ready(0)
    both(0, 0, tiles)
    forward(1)
    for g in range(1, len(groups)):
        forward(g + 1)
        ready(g)
        both(g, 0, tiles)

    tops = [jnp.max(mx[k], axis=0, keepdims=True) for k in range(nz)]
    top = functools.reduce(jnp.maximum, tops)
    parts = [jnp.exp2(t - top) for t in tops]
    total = sum(p * jnp.sum(tot[k], axis=0, keepdims=True) for k, p in enumerate(parts))
    delta = sum(p * jnp.sum(dl[k], axis=0, keepdims=True) for k, p in enumerate(parts))
    inv = 1.0 / total
    delta = delta * inv

    def settle(k, r):
        f = parts[group_of[k, r]] * inv
        rs = rows_of(k, r)
        for h in range(heads):
            ls = slice(h * queries, (h + 1) * queries)
            pr = S[rs, ls] * f[:, ls]
            pT[rs, ls] = pr.astype(BF16)
            dsT[rs, ls] = (pr * (dP[rs, ls] - delta[:, ls]) * scale).astype(BF16)

    def step_piece(k, r):
        rs = rows_of(k, r)
        ds, pb = dsT[rs, :], pT[rs, :]
        v = dot(ds, ext[:, 0:LATENT]) + dot(pb, back[...])
        t = dot(ds, ext[:, LATENT:width])
        n = quarter // 2
        for c in range(2):
            for xx in range(2):
                i = c * half + xx * quarter
                for j in range(LATENT // 128):
                    cols = slice(j * 128, (j + 1) * 128)
                    D[k, r, c, xx, j * quarter : (j + 1) * quarter, :] = v[i : i + quarter, cols]
                tail = jnp.concatenate([t[i : i + n], t[i + n : i + quarter]], axis=1)
                D[k, r, c, xx, LATENT // 128 * quarter :, :] = tail

    parts_of = [((k, r),) for k in range(nz - 1, nz - 1, -1) for r in (1, 0)]
    parts_of += [((k, 1), (k, 0)) for k in range(nz - 1, -1, -1)]

    def core_copy(i):
        k, r = parts_of[i][0]
        at_ = (k,) if len(parts_of[i]) > 1 else (k, r)
        return remote(csnd.at[at_], crcv.at[at_], c_send.at[0], c_recv.at[i], c_dev)

    plane = [(1, xp, y_dev), (0, oxp, x_dev), (1, oxp, xy_dev)]

    def plane_copy(k, i):
        return remote(
            psnd.at[k, i], prcv.at[k, i], p_send.at[0], p_recv.at[k], plane[i][2]
        )

    def z_copy(k):
        return remote(zsnd.at[k], zrcv.at[k], z_send.at[0], z_recv.at[0], z_devs[k])

    def chip_sum(k, r, xx):
        return D[k, r, core, xx] + crcv[k, r, xx].astype(F32)

    def step_d(i):
        then = list(parts_of[i + 1]) if i + 1 < len(parts_of) else []
        for b in parts_of[i]:
            step_piece(*b)
            if then:
                settle(*then.pop(0))
        for b in then:
            settle(*b)
        for k, r in parts_of[i]:
            csnd[k, r] = D[k, r, oc].astype(BF16)
        go(core_copy(i))

    def step_e(i):
        core_copy(i).wait_recv()
        for j in (2, 0, 1):
            for k, r in parts_of[i]:
                if plane[j][0] == r:
                    psnd[k, j] = chip_sum(k, r, plane[j][1]).astype(BF16)
                    go(plane_copy(k, j))

    def step_f(k):
        remote(prcv.at[k], prcv.at[k], p_send.at[0], p_recv.at[k], c_dev).wait_recv()
        u = chip_sum(k, 0, xp)
        for i in range(3):
            u = u + prcv[k, i].astype(F32)
        if k:
            zsnd[k] = u.astype(BF16)
            go(z_copy(k))
        return u

    def grad_ext(h):
        cols = slice(h * queries, (h + 2) * queries)
        g = dot(cT[...], dsT[:, cols])
        extT[0:LATENT, cols] = g[0:LATENT].astype(BF16)
        hi = g[LATENT:width]
        ropes = [hi[:, i * queries : (i + 1) * queries] * factor for i in range(2)]
        dqr_ref[:, h * ROPE : (h + 2) * ROPE] = jnp.concatenate(ropes, axis=0).T.astype(BF16)

    def grad_nope(h):
        for i in range(h, h + 2):
            cols = slice(i * NOPE, (i + 1) * NOPE)
            d = dot(upkT[cols, :], extT[0:LATENT, i * queries : (i + 1) * queries]) * factor
            dqn_ref[:, cols] = d.T.astype(BF16)

    todo = [functools.partial(grad_ext, 0)]
    for h in range(2, heads, 2):
        todo += [functools.partial(grad_ext, h), functools.partial(grad_nope, h - 2)]
    todo += [functools.partial(grad_nope, heads - 2)]

    def some(n):
        for _ in range(n):
            if todo:
                todo.pop(0)()

    for b in parts_of[0]:
        settle(*b)
    waiting = list(range(nz - 1, 0, -1))
    done = 0
    for i in range(len(parts_of)):
        step_d(i)
        while done < i and (len(parts_of[done + 1]) > 1 or done + 1 < i):
            step_e(done)
            done += 1
        if nz > 4 and i > nz:
            step_f(waiting.pop(0))
    some(1)
    for i in range(done, len(parts_of) - 1):
        step_e(i)
    for i, k in enumerate(waiting):
        if 1 and i == 2:
            step_e(len(parts_of) - 1)
        some((1, 1, 1)[i] if i < len((1, 1, 1)) else 0)
        step_f(k)
    some(2)
    v = step_f(0)
    if nz > 1:
        others = zrcv.at[1:nz]
        remote(others, others, z_send.at[0], z_recv.at[0], c_dev).wait_recv()
    for k in range(nz - 1, 0, -1):
        v = v + zrcv[k].astype(F32)
    if ngroups > 1:
        wsnd[...] = v.astype(BF16)
        for k in range(1, ngroups):
            go(remote(wsnd, wrcv.at[xg], w_send.at[k], w_recv.at[xg], g_devs[k]))
        wrcv[xg] = v.astype(BF16)
        for k in range(1, ngroups):
            remote(wsnd, wrcv.at[xgs[k]], w_send.at[k], w_recv.at[xgs[k]], g_devs[k]).wait_recv()
        v = wrcv[0].astype(F32)
        for i in range(1, ngroups):
            v = v + wrcv[i].astype(F32)
    fin[core * 2 + xp] = v.astype(BF16)
    here = fin.at[core * 2 + xp]
    last = [x_dev, xc_dev, c_dev]
    for dev in last:
        go(remote(here, here, f_send.at[0], f_recv.at[0], dev))
    some(len(todo))
    sent(land.at[0 : 2 * nz - 1], g_send.at[0])
    sent(csnd, c_send.at[0])
    sent(psnd, p_send.at[0])
    if nz > 1:
        sent(zsnd.at[1:nz], z_send.at[0])
    for k in range(1, ngroups):
        sent(wsnd, w_send.at[k])
    remote(fin.at[0:3], fin.at[0:3], f_send.at[0], f_recv.at[0], c_dev).wait_recv()
    quarters = [fin[i].astype(F32) for i in range(4)]
    for j in range(LATENT // 128):
        rs = slice(j * quarter, (j + 1) * quarter)
        tall = jnp.concatenate([q[rs] for q in quarters], axis=0)
        dc_ref[j * 128 : (j + 1) * 128, :] = tall.T.astype(BF16)
    rs = slice(LATENT // 128 * quarter, quarter * width // 128)
    tails = [q[rs, i * ROPE : (i + 1) * ROPE] for q in quarters for i in range(2)]
    dc_ref[LATENT:width, :] = jnp.concatenate(tails, axis=0).T.astype(BF16)
    sent(fin.at[0:3], f_send.at[0])


def finish(a, b, c, oa, ob, oc, sem):
    copies = [
        pltpu.make_async_copy(src, dst, sem.at[i])
        for i, (src, dst) in enumerate(((b, ob), (a, oa), (c, oc)))
    ]
    for copy in copies:
        copy.start()
    for copy in copies:
        copy.wait()


def solution(mesh):
    seq, head = mesh.shape["seq"], mesh.shape["head"]
    nz, nx = seq // 2, head // 2

    def per_device(cache, qn, qr, se, off, uk, uv, go):
        own, width = cache.shape
        keys = own * seq
        prow = own // 4 * width // 128
        queries = qn.shape[0]
        heads = qn.shape[1] // NOPE
        rows = heads * queries
        vm = pltpu.VMEM
        dma = pltpu.SemaphoreType.DMA
        vspec = pl.BlockSpec(memory_space=pltpu.VMEM)
        hspec = pl.BlockSpec(memory_space=pl.ANY)
        shapes = ((width, own), qn.shape, qr.shape)
        out = pl.pallas_call(
            functools.partial(kernel, nz, nx),
            out_shape=tuple(vm(s, BF16) for s in shapes),
            in_specs=[hspec] * 8,
            out_specs=(vspec, vspec, vspec),
            scratch_shapes=[
                vm((width, own), BF16), vm(qr.shape, BF16),
                vm((1, queries), jnp.int32), pltpu.SMEM(off.shape, jnp.int32),
                vm((2 * (queries + LATENT), qn.shape[1]), BF16),
                vm((seq, width, own), BF16), vm((keys, width), BF16), vm((width, keys), BF16),
                vm((width, rows), BF16), vm((rows, width), BF16),
                vm((LATENT, rows), BF16), vm((rows, LATENT), BF16),
                vm((heads * NOPE, LATENT), BF16),
                vm((keys, rows), F32), vm((keys, rows), F32),
                vm((keys, rows), BF16), vm((keys, rows), BF16),
                vm((nz, 8, rows), F32), vm((nz, 8, rows), F32), vm((nz, 8, rows), F32),
                vm((nz, 2, 2, 2, prow, 128), F32),
                vm((nz, 2, 2, prow, 128), BF16), vm((nz, 2, 2, prow, 128), BF16),
                vm((nz, 3, prow, 128), BF16), vm((nz, 3, prow, 128), BF16),
                vm((nz, prow, 128), BF16), vm((nz, prow, 128), BF16),
                vm((prow, 128), BF16), vm((nx // 2, prow, 128), BF16),
                vm((4, prow, 128), BF16),
                dma((5,)), dma((1,)), dma((4 * nz - 2,)), dma((1,)), dma((nz,)),
                dma((1,)), dma((nz,)), dma((1,)), dma((1,)),
                dma((nx // 2,)), dma((nx // 2,)), dma((1,)), dma((1,)),
            ],
            compiler_params=pltpu.CompilerParams(
                collective_id=0, has_side_effects=True, vmem_limit_bytes=58 * 1024 * 1024
            ),
        )(cache.T, qn, qr, se.reshape(1, -1), off, uk, uv, go)
        dc, dqn, dqr = pl.pallas_call(
            finish,
            out_shape=tuple(jax.ShapeDtypeStruct(s, BF16) for s in shapes),
            in_specs=[vspec] * 3,
            out_specs=(hspec,) * 3,
            scratch_shapes=[dma((3,))],
            compiler_params=pltpu.CompilerParams(vmem_limit_bytes=1024 * 1024),
        )(*out)
        return dc.T, dqn, dqr

    in_specs = (
        P("seq", None), P("seq", "head"), P("seq", "head"), P("seq"), P("seq"),
        P(None, "head"), P(None, "head"), P("seq", "head"),
    )
    out_specs = (P("seq", None), P("seq", "head"), P("seq", "head"))
    return jax.shard_map(
        per_device, mesh=mesh, in_specs=in_specs, out_specs=out_specs, check_vma=False
    )
```
